32 devices in a mesh: grp: 4 (over y, x), tile: 8 (over z, core).
Axes of the slice: x: 2, y: 2, z: 4, core: 2. Of those that a mesh axis runs over, the one named last changes fastest.
Arguments:
- base_rhs: float32 [1024, 4096], P('grp', 'tile'), may hold values from -6 to 6
- depth: float32 [1024, 4096], P('grp', 'tile'), may hold values from 0.25 to 2
- ssh_prev: float32 [1024, 4096], P('grp', 'tile'), may hold values from -6 to 6
- currents: float32 [2, 1024, 4096], P(None, 'grp', 'tile'), may hold values from -3 to 3
- land_blocks: int32 [128, 512], P('grp', 'tile'), may hold values 0 or 1
- ice_thick: float32 [2, 256, 4096], P(None, 'grp', 'tile'), may hold values from 0.25 to 4
- ice_blocks: int32 [2, 32, 512], P(None, 'grp', 'tile'), may hold values 0 or 1
- ice_vel: float32 [2, 2, 256, 4096], P(None, None, 'grp', 'tile'), may hold values from -3 to 3
- ice_stress: float32 [3, 2, 256, 4096], P(None, None, 'grp', 'tile'), may hold values from -5 to 5
- wind: float32 [2, 2, 256, 4096], P(None, None, 'grp', 'tile'), may hold values from -6 to 6
Outputs:
- ssh: float32 [1024, 4096], P('grp', 'tile')
- ice_vel_out: float32 [2, 2, 256, 4096], P(None, None, 'grp', 'tile')
- ice_stress_out: float32 [3, 2, 256, 4096], P(None, None, 'grp', 'tile')
The draws below stay inside these ranges and needn't reach their ends.
All inputs are finite; a program needn't handle non-finite values. No bound on the sum of `land_blocks` or of `ice_blocks` on one device may be relied on, other than what follows from the above.
Results may differ from the reference program's by a relative error of at most 0.0001.
Values sent between devices are 32-bit elements; how exact they have to be, the bound alone decides.
A program may use at most 64 MiB of HBM per device.

```python
import math
import jax
import jax.numpy as jnp

BS = 8
NSUB = 8
ITERS = 3
NX = 1024
NY = 4096
NXI = 256


def set_ends(values, own_key, least, largest):
    index_at = [jax.random.randint(jax.random.fold_in(own_key, axis), (), 0, length) for axis, length in enumerate(values.shape)]
    widest = values.shape.index(max(values.shape))
    beside = index_at[:widest] + [(index_at[widest] + 1) % values.shape[widest]] + index_at[widest + 1:]
    return values.at[tuple(index_at)].set(least).at[tuple(beside)].set(largest)


def level_of(key, extent, split, smallest, high):
    loudness = 1.0
    for position, shards_of in split:
        heights = jax.random.uniform(jax.random.fold_in(jax.random.fold_in(key, 6), position), (shards_of,), jnp.float32, smallest / len(split), high / len(split))
        loudness = loudness * jnp.repeat(jnp.exp(heights), extent[position] // shards_of).reshape((-1,) + (1,) * (len(extent) - 1 - position))
    return loudness


def bell_draw(rng, dims, scale, reach, pieces=(), held_as=jnp.bfloat16):
    level = level_of(rng, dims, pieces, -0.22, 0.18) if pieces else 1.0
    entries = jax.random.normal(rng, dims, jnp.float32) * scale * level
    return jnp.minimum(jnp.maximum(entries, -reach), reach).astype(held_as)


def setup_inputs(seed: int = 0) -> dict:
    key_list = jax.random.split(jax.random.key(seed), 11)
    base_rhs = bell_draw(key_list[0], (NX, NY), 1.0, 6.0, ((0, 4), (1, 8)), jnp.float32)
    depth = jnp.clip(jnp.exp(math.log(2.0) - 2.0794415 * jax.random.uniform(key_list[1], (NX, NY), jnp.float32) ** level_of(key_list[1], (NX, NY), ((0, 4), (1, 8)), -0.2, 0.2)), 0.25, 2.0)
    ssh_prev = bell_draw(key_list[2], (NX, NY), 1.0, 6.0, ((0, 4), (1, 8)), jnp.float32)
    currents = bell_draw(key_list[3], (2, NX, NY), 0.5, 3.0, ((1, 4), (2, 8)), jnp.float32)
    land_blocks = set_ends((jax.random.randint(key_list[4], (NX // BS, NY // BS), 0, 4) < 3).astype(jnp.int32), jax.random.fold_in(key_list[4], 1), 0, 1)
    ice_thick = jnp.clip(jnp.exp(math.log(4.0) - 2.7725887 * jax.random.uniform(key_list[5], (2, NXI, NY), jnp.float32) ** level_of(key_list[5], (2, NXI, NY), ((1, 4), (2, 8)), -0.2, 0.2)), 0.25, 4.0)
    ice_blocks = set_ends((jax.random.randint(key_list[6], (2, NXI // BS, NY // BS), 0, 4) < 3).astype(jnp.int32), jax.random.fold_in(key_list[6], 1), 0, 1)
    ice_vel = bell_draw(key_list[7], (2, 2, NXI, NY), 0.5, 3.0, ((2, 4), (3, 8)), jnp.float32)
    ice_stress = bell_draw(key_list[8], (3, 2, NXI, NY), 1.0, 5.0, ((2, 4), (3, 8)), jnp.float32)
    wind = bell_draw(key_list[9], (2, 2, NXI, NY), 1.0, 6.0, ((2, 4), (3, 8)), jnp.float32)
    return dict(base_rhs=base_rhs, depth=depth, ssh_prev=ssh_prev, currents=currents, land_blocks=land_blocks, ice_thick=ice_thick, ice_blocks=ice_blocks, ice_vel=ice_vel, ice_stress=ice_stress, wind=wind)


DAMP = 0.05
RELAX = 0.2
STRENGTH = 0.5
DRAG = 1.0
STEP = 0.5

def strain_rates(u_pad, v_pad):
    du_dx = u_pad[..., 1:, :-1] - u_pad[..., :-1, :-1]
    du_dy = u_pad[..., :-1, 1:] - u_pad[..., :-1, :-1]
    dv_dx = v_pad[..., 1:, :-1] - v_pad[..., :-1, :-1]
    dv_dy = v_pad[..., :-1, 1:] - v_pad[..., :-1, :-1]
    return (du_dx + dv_dy, du_dx - dv_dy, du_dy + dv_dx)

def relax_stress(previous, strength, div_rate, tens_rate, shear_rate):
    deformation = jnp.sqrt(div_rate * div_rate + tens_rate * tens_rate + shear_rate * shear_rate + 1.0)
    relax_scale = 1.0 / (1.0 + RELAX)
    div_part = (previous[0] + RELAX * strength * (div_rate / deformation - 1.0)) * relax_scale
    tens_part = (previous[1] + RELAX * strength * tens_rate / deformation) * relax_scale
    shear_part = (previous[2] + RELAX * strength * shear_rate / deformation) * relax_scale
    return jnp.stack([div_part, tens_part, shear_part])

def along_rows(field):
    return field[..., 1:, 1:] - field[..., :-1, 1:]

def along_cols(field):
    return field[..., 1:, 1:] - field[..., 1:, :-1]

def stress_force(stress_pad):
    force_x = 0.5 * along_rows(stress_pad[0] + stress_pad[1]) + along_cols(stress_pad[2])
    force_y = 0.5 * along_cols(stress_pad[0] - stress_pad[1]) + along_rows(stress_pad[2])
    return jnp.stack([force_x, force_y])

def momentum(velocity, force, ice_mass, ice_cover, wind, ocean_flow):
    return ice_cover * (ice_mass * velocity + STEP * (force + wind + DRAG * ocean_flow)) / (ice_mass + STEP * DRAG)

def face_weights(depth_pad):
    centre = depth_pad[1:-1, 1:-1]
    return (centre * depth_pad[2:, 1:-1], centre * depth_pad[:-2, 1:-1], centre * depth_pad[1:-1, 2:], centre * depth_pad[1:-1, :-2])

def apply_operator(field_pad, weights):
    field = field_pad[1:-1, 1:-1]
    north_weight, south_weight, east_weight, west_weight = weights
    return DAMP * field + north_weight * (field - field_pad[2:, 1:-1]) + south_weight * (field - field_pad[:-2, 1:-1]) + east_weight * (field - field_pad[1:-1, 2:]) + west_weight * (field - field_pad[1:-1, :-2])

def expand(blocks):
    return jnp.repeat(jnp.repeat(blocks, BS, axis=-2), BS, axis=-1).astype(jnp.float32)

def reference(base_rhs, depth, ssh_prev, currents, land_blocks, ice_thick, ice_blocks, ice_vel, ice_stress, wind):
    wet_cells = expand(land_blocks)
    ice_cover = expand(ice_blocks)
    strength = STRENGTH * ice_thick * ice_cover
    ice_mass = ice_thick * ice_cover + 1.0
    ocean_flow = jnp.stack([currents[:, :NXI], currents[:, NX - NXI:]], axis=1)
    velocity = ice_vel
    stress = ice_stress
    for subcycle in range(NSUB):
        vel_pad = jnp.pad(velocity, ((0, 0), (0, 0), (1, 1), (1, 1)))
        strain = strain_rates(vel_pad[0], vel_pad[1])
        div_rate = strain[0][:, 1:, 1:]
        tens_rate = strain[1][:, 1:, 1:]
        shear_rate = strain[2][:, 1:, 1:]
        stress = relax_stress(stress, strength, div_rate, tens_rate, shear_rate)
        stress_pad = jnp.pad(stress, ((0, 0), (0, 0), (1, 0), (1, 0)))
        velocity = momentum(velocity, stress_force(stress_pad), ice_mass, ice_cover, wind, ocean_flow)
    ice_drag = DRAG * ice_cover * (velocity - ocean_flow)
    ocean_drag = jnp.zeros((2, NX, NY), jnp.float32)
    ocean_drag = ocean_drag.at[:, :NXI].set(ice_drag[:, 0]).at[:, NX - NXI:].set(ice_drag[:, 1])
    forcing_pad = jnp.pad(jnp.stack([ocean_drag[0], ocean_drag[1], depth * wet_cells]), ((0, 0), (1, 1), (1, 1)))
    spread = forcing_pad[0, 1:-1, 1:-1] - forcing_pad[0, :-2, 1:-1] + (forcing_pad[1, 1:-1, 1:-1] - forcing_pad[1, 1:-1, :-2])
    forcing = wet_cells * (base_rhs + spread)
    weights = face_weights(forcing_pad[2])
    diagonal = DAMP + weights[0] + weights[1] + weights[2] + weights[3]
    solution = ssh_prev
    residual = forcing - apply_operator(jnp.pad(solution, 1), weights)
    precond = residual / diagonal
    direction = precond
    precond_norm = jnp.sum(residual * precond)
    for iteration in range(ITERS):
        applied = apply_operator(jnp.pad(direction, 1), weights)
        step_size = precond_norm / jnp.sum(direction * applied)
        solution = solution + step_size * direction
        residual = residual - step_size * applied
        precond = residual / diagonal
        norm_next = jnp.sum(residual * precond)
        direction = precond + norm_next / precond_norm * direction
        precond_norm = norm_next
    return (solution, velocity, stress)
```

```python
import functools

import jax
import jax.numpy as jnp
from jax import lax
from jax.experimental import pallas as pl
from jax.experimental.pallas import tpu as pltpu
from jax.sharding import PartitionSpec as P

BS = 8
NSUB = 8

DAMP = 0.05
RELAX = 0.2
STRENGTH = 0.5
DRAG = 1.0
STEP = 0.5

MESH = pl.DeviceIdType.MESH
F32 = jnp.float32
T = 8
L = 128
W = 12
TOP = 2 * T


def lanes(rows, width):
    return lax.broadcasted_iota(jnp.int32, (rows, width), 1)


def right(x):
    return pltpu.roll(x, x.shape[1] - 1, 1)


def left(x):
    return pltpu.roll(x, 1, 1)


def rows_of(shape):
    return lax.broadcasted_iota(jnp.int32, shape, 0)


def above(prev, here):
    return pltpu.roll(jnp.where(rows_of(here.shape) == T - 1, prev, here), 1, 0)


def below(here, after):
    return pltpu.roll(jnp.where(rows_of(here.shape) == 0, after, here), T - 1, 0)


def kernel(
    groups,
    tiles,
    base_in,
    depth_in,
    ssh_in,
    cur_in,
    land_ref,
    thick_in,
    ice_ref,
    vel_in,
    stress_in,
    wind_in,
    ssh_out,
    vel_out,
    stress_out,
    vel,
    st,
    wind,
    flow,
    h,
    kk,
    pp,
    qq,
    g,
    x,
    b,
    gd,
    v0,
    v1,
    v2,
    w0,
    w1,
    w2,
    wet,
    cover,
    pack_s,
    pack_r,
    opack_s,
    opack_r,
    sp,
    back,
    top_in,
    bot_in,
    red_s,
    red_r,
    red2_s,
    red2_r,
    load_sem,
    flow_send,
    flow_recv,
    row_send,
    row_recv,
    col_send,
    col_recv,
    back_send,
    back_recv,
    edge_send,
    edge_recv,
    red_send,
    red_recv,
    red2_send,
    red2_recv,
    out_sem,
):
    gi = lax.axis_index("grp")
    ti = lax.axis_index("tile")
    rows, cols = thick_in.shape[1], thick_in.shape[2]
    orows = base_in.shape[0]
    wide = cols + L
    end = TOP + rows
    oend = TOP + orows

    loads = []

    def load(src, dst):
        copy = pltpu.make_async_copy(src, dst, load_sem.at[len(loads)])
        copy.start()
        loads.append(copy)
        return copy

    load_thick = load(thick_in, h.at[:, TOP:end, 0:cols])
    load_depth = load(depth_in, g.at[TOP:oend, 0:cols])
    load_x = load(ssh_in, x.at[TOP:oend, 0:cols])
    load_b = load(base_in, b.at[TOP:oend, 0:cols])
    load_vel = load(vel_in, vel.at[:, :, TOP:end, 0:cols])
    load_st = load(stress_in, st.at[:, :, TOP:end, 0:cols])
    load_wind = load(wind_in, wind.at[:, :, TOP:end, 0:cols])

    def clear(ref, top, last, total):
        ref[..., 0:top, :] = jnp.zeros(ref.shape[:-2] + (top, wide), F32)
        ref[..., last:total, :] = jnp.zeros(ref.shape[:-2] + (total - last, wide), F32)
        ref[..., top:last, cols:wide] = jnp.zeros(ref.shape[:-2] + (last - top, L), F32)

    for ref in (vel, st, wind, flow, h):
        clear(ref, TOP, end, end + TOP)
    for ref in (g, x, b):
        clear(ref, TOP, oend, oend + TOP)
    for ref in (pack_r, opack_r):
        ref[...] = jnp.zeros_like(ref)

    barrier = pltpu.get_barrier_semaphore()
    for d in range(1, groups):
        pl.semaphore_signal(
            barrier, inc=1, device_id=(lax.rem(gi + d, groups), ti), device_id_type=MESH
        )
    for d in range(1, tiles):
        pl.semaphore_signal(
            barrier, inc=1, device_id=(gi, lax.rem(ti + d, tiles)), device_id_type=MESH
        )

    def blocks(ref, out, count):
        width = ref.shape[-1]
        row = lax.broadcasted_iota(jnp.int32, (width, cols), 0)
        spread = (row == lax.shift_right_logical(lanes(width, cols), 3)).astype(F32)
        values = ref[...].reshape((count, width)).astype(F32)
        out[...] = jnp.dot(values, spread, preferred_element_type=F32)

    blocks(land_ref, wet, land_ref.shape[0])
    for c in range(2):
        row = lax.broadcasted_iota(jnp.int32, (cols // BS, cols), 0)
        spread = (row == lax.shift_right_logical(lanes(cols // BS, cols), 3)).astype(F32)
        cover[c] = jnp.dot(ice_ref[c].astype(F32), spread, preferred_element_type=F32)

    pl.semaphore_wait(barrier, groups + tiles - 2)

    def flow_copy(cap, target):
        lo = max(0, rows * target - T)
        hi = min(rows * groups, rows * target + rows + T)
        start = TOP + lo - rows * target
        src = cur_in.at[:, lo:hi, :]
        dst = flow.at[:, cap, start : start + hi - lo, 0:cols]
        return src, dst

    homes = (0, groups - 1)
    for cap, home in enumerate(homes):

        @pl.when(gi == home)
        def _():
            order = sorted(range(groups), key=lambda k: -abs(k - home))
            for target in order:
                src, dst = flow_copy(cap, target)
                if target == home:
                    pltpu.make_async_copy(src, dst, flow_recv.at[cap]).start()
                else:
                    pltpu.make_async_remote_copy(
                        src_ref=src,
                        dst_ref=dst,
                        send_sem=flow_send.at[target],
                        recv_sem=flow_recv.at[cap],
                        device_id=(target, ti),
                        device_id_type=MESH,
                    ).start()

    def row_copies(which):
        out = []
        fields = (
            (vel_in, vel, rows, end),
            (stress_in, st, rows, end),
            (wind_in, wind, rows, end),
            (ssh_in, x, orows, oend),
            (base_in, b, orows, oend),
            (h, h, None, end),
            (g, g, None, oend),
        )
        for k, (src, dst, length, last) in enumerate(fields):
            if (k >= 5) != which:
                continue
            origin = TOP if length is None else 0
            span = (last - TOP) if length is None else length
            lead = (slice(None),) * (len(src.shape) - 2)
            for way in range(2):
                from_row = origin + span - T if way == 0 else origin
                to_row = TOP - T if way == 0 else last
                out.append(
                    (
                        way,
                        pltpu.make_async_remote_copy(
                            src_ref=src.at[lead + (slice(from_row, from_row + T), slice(0, cols))],
                            dst_ref=dst.at[lead + (slice(to_row, to_row + T), slice(0, cols))],
                            send_sem=row_send.at[2 * k + way],
                            recv_sem=row_recv.at[2 * k + way],
                            device_id=(
                                lax.rem(gi + (1 if way == 0 else groups - 1), groups),
                                ti,
                            ),
                            device_id_type=MESH,
                        ),
                    )
                )
        return out

    def edge(way, index, count):
        sends = index < count - 1 if way == 0 else index > 0
        receives = index > 0 if way == 0 else index < count - 1
        return sends, receives

    early = row_copies(False)
    for way, copy in early:
        pl.when(edge(way, gi, groups)[0])(copy.start)

    load_thick.wait()

    def cover_chunk(k, _):
        for c in range(2):
            at = (c, pl.ds(pl.multiple_of(TOP + k * T, T), T), pl.ds(0, cols))
            h[at] = h[at] * cover[c, pl.ds(k, 1), :]
        return 0

    lax.fori_loop(0, rows // T, cover_chunk, 0)
    load_depth.wait()

    def wet_chunk(k, _):
        at = (pl.ds(pl.multiple_of(TOP + k * T, T), T), pl.ds(0, cols))
        g[at] = g[at] * wet[pl.ds(k, 1), :]
        return 0

    lax.fori_loop(0, orows // T, wet_chunk, 0)
    late = row_copies(True)
    for way, copy in late:
        pl.when(edge(way, gi, groups)[0])(copy.start)
    load_vel.wait()
    load_st.wait()
    load_wind.wait()
    load_x.wait()
    load_b.wait()
    for way, copy in early + late:
        pl.when(edge(way, gi, groups)[1])(copy.wait_recv)

    lane = lanes(T, L)

    def col_copies(src, dst, base):
        out = []
        for way in range(2):
            out.append(
                (
                    way,
                    pltpu.make_async_remote_copy(
                        src_ref=src.at[way],
                        dst_ref=dst.at[way],
                        send_sem=col_send.at[base + way],
                        recv_sem=col_recv.at[base + way],
                        device_id=(gi, lax.rem(ti + (1 if way == 0 else tiles - 1), tiles)),
                        device_id_type=MESH,
                    ),
                )
            )
        return out

    def packed(values):
        after = jnp.zeros((T, L), F32)
        before = jnp.zeros((T, L), F32)
        for f, (first, last) in enumerate(values):
            here = (lane >= W * f) & (lane < W * f + W)
            after = jnp.where(here, pltpu.roll(last, (W * f + W) % L, 1), after)
            before = jnp.where(here, pltpu.roll(first, W * f, 1) if f else first, before)
        return after, before

    def unpacked(from_before, from_after, f):
        low = pltpu.roll(from_before, (L - W - W * f) % L, 1)
        high = pltpu.roll(from_after, (L - W * f) % L, 1) if f else from_after
        return jnp.where(lane < W, high, jnp.where(lane >= L - W, low, 0.0))

    ochunks = orows // T + 2
    ichunks = rows // T + 2

    def opack_chunk(k, _):
        at = pl.ds(pl.multiple_of(T + k * T, T), T)
        to = pl.ds(pl.multiple_of(k * T, T), T)
        after, before = packed(
            [(ref[at, pl.ds(0, L)], ref[at, pl.ds(cols - L, L)]) for ref in (g, x, b)]
        )
        opack_s[0, to, :] = after
        opack_s[1, to, :] = before
        return 0

    lax.fori_loop(0, ochunks, opack_chunk, 0)
    ocols = col_copies(opack_s, opack_r, 0)
    for way, copy in ocols:
        pl.when(edge(way, ti, tiles)[0])(copy.start)

    for target in range(groups):

        @pl.when(gi == target)
        def _():
            for cap, home in enumerate(homes):
                src, dst = flow_copy(cap, target)
                if target == home:
                    pltpu.make_async_copy(src, dst, flow_recv.at[cap]).wait()
                else:
                    pltpu.make_async_remote_copy(
                        src_ref=src,
                        dst_ref=dst,
                        send_sem=flow_send.at[target],
                        recv_sem=flow_recv.at[cap],
                        device_id=(home, ti),
                        device_id_type=MESH,
                    ).wait_recv()

    def ice_fields(c):
        return (
            vel.at[0, c],
            vel.at[1, c],
            st.at[0, c],
            st.at[1, c],
            st.at[2, c],
            h.at[c],
            wind.at[0, c],
            wind.at[1, c],
            flow.at[0, c],
            flow.at[1, c],
        )

    def pack_chunk(k, _):
        at = pl.ds(pl.multiple_of(T + k * T, T), T)
        to = pl.ds(pl.multiple_of(k * T, T), T)
        for c in range(2):
            after, before = packed(
                [(ref[at, pl.ds(0, L)], ref[at, pl.ds(cols - L, L)]) for ref in ice_fields(c)]
            )
            pack_s[0, c, to, :] = after
            pack_s[1, c, to, :] = before
        return 0

    lax.fori_loop(0, ichunks, pack_chunk, 0)
    icols = col_copies(pack_s, pack_r, 2)
    for way, copy in icols:
        pl.when(edge(way, ti, tiles)[0])(copy.start)

    for way, copy in ocols:
        pl.when(edge(way, ti, tiles)[1])(copy.wait_recv)

    def ounpack_chunk(k, _):
        at = pl.ds(pl.multiple_of(T + k * T, T), T)
        to = pl.ds(pl.multiple_of(k * T, T), T)
        for f, ref in enumerate((g, x, b)):
            ref[at, pl.ds(cols, L)] = unpacked(opack_r[0, to, :], opack_r[1, to, :], f)
        return 0

    lax.fori_loop(0, ochunks, ounpack_chunk, 0)

    for way, copy in icols:
        pl.when(edge(way, ti, tiles)[1])(copy.wait_recv)

    def unpack_chunk(k, _):
        at = pl.ds(pl.multiple_of(T + k * T, T), T)
        to = pl.ds(pl.multiple_of(k * T, T), T)
        for c in range(2):
            for f, ref in enumerate(ice_fields(c)):
                ref[at, pl.ds(cols, L)] = unpacked(pack_r[0, c, to, :], pack_r[1, c, to, :], f)
            thick = h[c, at, :]
            mass = thick + 1.0
            inverse = jnp.where(thick > 0.0, 1.0 / (mass + STEP * DRAG), 0.0)
            q = STEP * inverse
            kk[c, at, :] = (RELAX * STRENGTH / (1.0 + RELAX)) * thick
            pp[c, at, :] = mass * inverse
            qq[c, at, :] = q
            for comp in range(2):
                wind[comp, c, at, :] = q * (wind[comp, c, at, :] + DRAG * flow[comp, c, at, :])
        return 0

    lax.fori_loop(0, ichunks, unpack_chunk, 0)

    keep = 1.0 / (1.0 + RELAX)

    def ice_chunk(k, _):
        r = pl.multiple_of(T + k * T, T)
        at = pl.ds(r, T)
        up = pl.ds(pl.multiple_of(r - T, T), T)
        down = pl.ds(pl.multiple_of(r + T, T), T)
        for c in range(2):
            u = vel[0, c, at, :]
            v = vel[1, c, at, :]
            du_dx = below(u, vel[0, c, down, :]) - u
            dv_dx = below(v, vel[1, c, down, :]) - v
            du_dy = right(u) - u
            dv_dy = right(v) - v
            ed = du_dx + dv_dy
            et = du_dx - dv_dy
            es = du_dy + dv_dx
            inverse = lax.rsqrt(ed * ed + et * et + es * es + 1.0)
            k0 = kk[c, at, :]
            k1 = k0 * inverse
            s0 = st[0, c, at, :] * keep + (k1 * ed - k0)
            s1 = st[1, c, at, :] * keep + k1 * et
            s2 = st[2, c, at, :] * keep + k1 * es
            st[0, c, at, :] = s0
            st[1, c, at, :] = s1
            st[2, c, at, :] = s2
            total = s0 + s1
            diff = s0 - s1
            total_up = above(st[0, c, up, :] + st[1, c, up, :], total)
            s2_up = above(st[2, c, up, :], s2)
            fx = 0.5 * (total - total_up) + (s2 - left(s2))
            fy = 0.5 * (diff - left(diff)) + (s2 - s2_up)
            p = pp[c, at, :]
            q = qq[c, at, :]
            vel[0, c, at, :] = p * u + (q * fx + wind[0, c, at, :])
            vel[1, c, at, :] = p * v + (q * fy + wind[1, c, at, :])
        return 0

    def subcycle(n, _):
        return lax.fori_loop(0, ichunks, ice_chunk, 0)

    lax.fori_loop(0, NSUB, subcycle, 0)

    sub = lax.broadcasted_iota(jnp.int32, (T, wide), 0)

    def drag(comp, c, where):
        return jnp.where(
            h[c, where, :] > 0.0, DRAG * (vel[comp, c, where, :] - flow[comp, c, where, :]), 0.0
        )

    def drag_chunk(k, _):
        r = pl.multiple_of(TOP + k * T, T)
        to = pl.ds(pl.multiple_of(k * T, T), T)
        for c in range(2):
            d0 = drag(0, c, pl.ds(r, T))
            d0_up = above(drag(0, c, pl.ds(pl.multiple_of(r - T, T), T)), d0)
            d0_up = jnp.where((sub == 0) & (k == 0), 0.0, d0_up)
            d1 = drag(1, c, pl.ds(r, T))
            sp[c, to, :] = (d0 - d0_up) + (d1 - left(d1))
        return 0

    lax.fori_loop(0, rows // T, drag_chunk, 0)
    for c in range(2):
        sp[c, rows : rows + T, :] = drag(0, c, pl.ds(end - T, T))

    outs = [
        pltpu.make_async_copy(vel.at[:, :, TOP:end, 0:cols], vel_out, out_sem.at[0]),
        pltpu.make_async_copy(st.at[:, :, TOP:end, 0:cols], stress_out, out_sem.at[1]),
    ]

    def back_copy(cap, source, target):
        return pltpu.make_async_remote_copy(
            src_ref=sp.at[cap],
            dst_ref=back.at[source],
            send_sem=back_send.at[cap],
            recv_sem=back_recv.at[source],
            device_id=(target, ti),
            device_id_type=MESH,
        )

    def to_top():
        return pltpu.make_async_remote_copy(
            src_ref=sp.at[0, rows - T : rows + T, :],
            dst_ref=top_in,
            send_sem=edge_send.at[0],
            recv_sem=edge_recv.at[0],
            device_id=(1, ti),
            device_id_type=MESH,
        )

    def to_bot():
        return pltpu.make_async_remote_copy(
            src_ref=sp.at[1, 0:T, :],
            dst_ref=bot_in,
            send_sem=edge_send.at[1],
            recv_sem=edge_recv.at[1],
            device_id=(groups - 2, ti),
            device_id_type=MESH,
        )

    pl.when(gi == groups - 1)(lambda: to_top().start())
    pl.when(gi == 0)(lambda: to_bot().start())
    for cap, home in enumerate(homes):
        for source in range(groups):

            @pl.when(gi == source)
            def _():
                if source == home:
                    pltpu.make_async_copy(
                        sp.at[cap], back.at[source], back_recv.at[source]
                    ).start()
                else:
                    back_copy(cap, source, home).start()

    for copy in outs:
        copy.start()

    for cap, home in enumerate(homes):

        @pl.when(gi == home)
        def _():
            for source in range(groups):
                if source == home:
                    pltpu.make_async_copy(
                        sp.at[cap], back.at[source], back_recv.at[source]
                    ).wait()
                else:
                    back_copy(cap, source, source).wait_recv()
            for source in range(groups):

                def add_chunk(k, _):
                    at = pl.ds(pl.multiple_of(TOP + source * rows + k * T, T), T)
                    b[at, :] = b[at, :] + back[source, pl.ds(pl.multiple_of(k * T, T), T), :]
                    return 0

                lax.fori_loop(0, rows // T, add_chunk, 0)
            for source in range(groups):
                row = TOP + (source + 1) * rows
                b[row : row + 1, :] = (
                    b[row : row + 1, :] - back[source, rows + T - 1 : rows + T, :]
                )

    @pl.when(gi == 1)
    def _():
        to_top().wait_recv()
        b[T:TOP, :] = b[T:TOP, :] + top_in[0:T, :]
        b[TOP : TOP + 1, :] = b[TOP : TOP + 1, :] - top_in[2 * T - 1 : 2 * T, :]

    @pl.when(gi == groups - 2)
    def _():
        to_bot().wait_recv()
        b[oend : oend + T, :] = b[oend : oend + T, :] + bot_in[...]

    zero = jnp.zeros((T, L), F32)

    def fold(value):
        total = value[:, 0:L]
        for j in range(1, cols // L):
            total = total + value[:, j * L : (j + 1) * L]
        return total

    def owned(k):
        return jnp.where((k >= 1) & (k <= orows // T), 1.0, 0.0).astype(F32)

    def around(ref, r):
        middle = ref[pl.ds(r, T), :]
        up = above(ref[pl.ds(pl.multiple_of(r - T, T), T), :], middle)
        down = below(middle, ref[pl.ds(pl.multiple_of(r + T, T), T), :])
        return (up + down) + (left(middle) + right(middle))

    for ref in (w0, w1, w2):
        ref[0:T, :] = jnp.zeros((T, wide), F32)
        ref[oend + T :, :] = jnp.zeros((T, wide), F32)

    def first_chunk(k, sums):
        r = pl.multiple_of(T + k * T, T)
        at = pl.ds(r, T)
        up, down = pl.ds(pl.multiple_of(r - T, T), T), pl.ds(pl.multiple_of(r + T, T), T)
        g0, gu, gw = g[at, :], g[up, :], g[down, :]
        x_0 = x[at, :]
        gx = g0 * x_0
        g_near = (above(gu, g0) + below(g0, gw)) + (left(g0) + right(g0))
        diag = DAMP + g0 * g_near
        near = (above(gu * x[up, :], gx) + below(gx, gw * x[down, :])) + (left(gx) + right(gx))
        r0 = jnp.where(g0 > 0.0, b[at, :], 0.0) - diag * x_0 + g0 * near
        inverse = 1.0 / diag
        z = r0 * inverse
        v0[at, :] = z
        w0[at, :] = g0 * z
        gd[at, :] = g0 * inverse
        return sums + owned(k) * fold(r0 * z)

    m0 = lax.fori_loop(0, ochunks, first_chunk, zero)

    def power(w_from, v_to, w_to):
        def chunk(k, sums):
            r = pl.multiple_of(T + k * T, T)
            at = pl.ds(r, T)
            near = around(w_from, r)
            v = gd[at, :] * near
            w = g[at, :] * v
            v_to[at, :] = v
            w_to[at, :] = w
            own = owned(k)
            return (
                sums[0] + own * fold(w_from[at, :] * near),
                sums[1] + own * fold(w * near),
            )

        return lax.fori_loop(0, ochunks, chunk, (zero, zero))

    m1, m2 = power(w0, v1, w1)
    m3, m4 = power(w1, v2, w2)

    def last_chunk(k, sums):
        r = pl.multiple_of(TOP + k * T, T)
        return sums + fold(w2[pl.ds(r, T), :] * around(w2, r))

    m5 = lax.fori_loop(0, orows // T, last_chunk, zero)

    row = lax.broadcasted_iota(jnp.int32, (T, L), 0)
    moments = zero
    for k, m in enumerate((m0, m1, m2, m3, m4, m5)):
        moments = jnp.where(row == k, jnp.sum(m, axis=0, keepdims=True), moments)

    def all_reduce(value, src, dst, send, recv, index, count, device):
        src[...] = value
        for d in range(1, count):
            pltpu.make_async_remote_copy(
                src_ref=src,
                dst_ref=dst.at[d],
                send_sem=send.at[d],
                recv_sem=recv.at[d],
                device_id=device(lax.rem(index + d, count)),
                device_id_type=MESH,
            ).start()
        for d in range(1, count):
            copy = pltpu.make_async_remote_copy(
                src_ref=src,
                dst_ref=dst.at[d],
                send_sem=send.at[d],
                recv_sem=recv.at[d],
                device_id=device(lax.rem(index + d, count)),
                device_id_type=MESH,
            )
            copy.wait()
        for d in range(1, count):
            value = value + dst[d]
        return value

    moments = all_reduce(
        moments, red_s, red_r, red_send, red_recv, ti, tiles, lambda k: (gi, k)
    )
    moments = all_reduce(
        moments, red2_s, red2_r, red2_send, red2_recv, gi, groups, lambda k: (k, ti)
    )
    total = jnp.sum(moments, axis=1, keepdims=True)
    nu = [total[k : k + 1, :] for k in range(6)]
    a = [nu[k] - nu[k + 1] for k in range(5)]

    tiny = 1e-12

    def safe(value, scale):
        ok = value > tiny * scale
        return jnp.where(ok, 1.0 / jnp.where(ok, value, 1.0), 0.0)

    i0 = safe(a[0], 0.0 * a[0])
    l10, l20 = a[1] * i0, a[2] * i0
    d1 = a[2] - l10 * a[1]
    i1 = safe(d1, a[2])
    e21 = a[3] - l20 * a[1]
    l21 = e21 * i1
    d2 = a[4] - l20 * a[2] - l21 * e21
    i2 = safe(d2, a[4])
    y0 = nu[0]
    y1 = nu[1] - l10 * y0
    y2 = nu[2] - l20 * y0 - l21 * y1
    c2 = y2 * i2
    c1 = y1 * i1 - l21 * c2
    c0 = y0 * i0 - l10 * c1 - l20 * c2

    def final_chunk(k, _):
        at = (pl.ds(pl.multiple_of(TOP + k * T, T), T), pl.ds(0, cols))
        x[at] = x[at] + (c0 * v0[at] + (c1 * v1[at] + c2 * v2[at]))
        return 0

    lax.fori_loop(0, orows // T, final_chunk, 0)
    last = pltpu.make_async_copy(x.at[TOP:oend, 0:cols], ssh_out, out_sem.at[2])
    last.start()

    for way, copy in early + late:
        pl.when(edge(way, gi, groups)[0])(copy.wait_send)
    for way, copy in ocols + icols:
        pl.when(edge(way, ti, tiles)[0])(copy.wait_send)
    for cap, home in enumerate(homes):

        @pl.when(gi == home)
        def _():
            for target in range(groups):
                if target != home:
                    src, dst = flow_copy(cap, target)
                    pltpu.make_async_remote_copy(
                        src_ref=src,
                        dst_ref=dst,
                        send_sem=flow_send.at[target],
                        recv_sem=flow_recv.at[cap],
                        device_id=(target, ti),
                        device_id_type=MESH,
                    ).wait_send()

        @pl.when(gi != home)
        def _():
            back_copy(cap, 0, home).wait_send()

    pl.when(gi == groups - 1)(lambda: to_top().wait_send())
    pl.when(gi == 0)(lambda: to_bot().wait_send())
    for copy in outs:
        copy.wait()
    last.wait()


def step(groups, tiles, *args):
    base_rhs, thick, ice_vel, ice_stress = args[0], args[5], args[7], args[8]
    orows, cols = base_rhs.shape
    rows = thick.shape[1]
    irows = rows + 2 * TOP
    erows = orows + 2 * TOP
    wide = cols + L
    any_spec = pl.BlockSpec(memory_space=pl.ANY)
    vmem = pl.BlockSpec(memory_space=pltpu.VMEM)
    dma = pltpu.SemaphoreType.DMA
    ice = pltpu.VMEM((2, irows, wide), F32)
    ocean = pltpu.VMEM((erows, wide), F32)
    return pl.pallas_call(
        functools.partial(kernel, groups, tiles),
        out_shape=(
            jax.ShapeDtypeStruct(base_rhs.shape, F32),
            jax.ShapeDtypeStruct(ice_vel.shape, F32),
            jax.ShapeDtypeStruct(ice_stress.shape, F32),
        ),
        in_specs=[any_spec] * 4 + [vmem, any_spec, vmem] + [any_spec] * 3,
        out_specs=(any_spec,) * 3,
        scratch_shapes=[
            pltpu.VMEM((2, 2, irows, wide), F32),
            pltpu.VMEM((3, 2, irows, wide), F32),
            pltpu.VMEM((2, 2, irows, wide), F32),
            pltpu.VMEM((2, 2, irows, wide), F32),
            ice,
            ice,
            ice,
            ice,
        ]
        + [ocean] * 10
        + [
            pltpu.VMEM((orows // BS, cols), F32),
            pltpu.VMEM((2, rows // BS, cols), F32),
            pltpu.VMEM((2, 2, rows + 2 * T, L), F32),
            pltpu.VMEM((2, 2, rows + 2 * T, L), F32),
            pltpu.VMEM((2, orows + 2 * T, L), F32),
            pltpu.VMEM((2, orows + 2 * T, L), F32),
            pltpu.VMEM((2, rows + T, wide), F32),
            pltpu.VMEM((groups, rows + T, wide), F32),
            pltpu.VMEM((2 * T, wide), F32),
            pltpu.VMEM((T, wide), F32),
            pltpu.VMEM((T, L), F32),
            pltpu.VMEM((tiles, T, L), F32),
            pltpu.VMEM((T, L), F32),
            pltpu.VMEM((groups, T, L), F32),
            dma((7,)),
            dma((groups,)),
            dma((2,)),
            dma((14,)),
            dma((14,)),
            dma((4,)),
            dma((4,)),
            dma((2,)),
            dma((groups,)),
            dma((2,)),
            dma((2,)),
            dma((tiles,)),
            dma((tiles,)),
            dma((groups,)),
            dma((groups,)),
            dma((3,)),
        ],
        compiler_params=pltpu.CompilerParams(
            collective_id=0, has_side_effects=True, vmem_limit_bytes=48 * 1024 * 1024
        ),
    )(*args)


def solution(mesh):
    grid = P("grp", "tile")
    plane = P(None, "grp", "tile")
    stack = P(None, None, "grp", "tile")
    return jax.shard_map(
        functools.partial(step, mesh.shape["grp"], mesh.shape["tile"]),
        mesh=mesh,
        in_specs=(grid, grid, grid, plane, grid, plane, plane, stack, stack, stack),
        out_specs=(grid, stack, stack),
        check_vma=False,
    )
```

```python
import functools

import jax
import jax.numpy as jnp
from jax import lax
from jax.experimental import pallas as pl
from jax.experimental.pallas import tpu as pltpu
from jax.sharding import PartitionSpec as P

BS = 8
NSUB = 8

DAMP = 0.05
RELAX = 0.2
STRENGTH = 0.5
DRAG = 1.0
STEP = 0.5

MESH = pl.DeviceIdType.MESH
F32 = jnp.float32
T = 8
L = 128
W = 12
TOP = 2 * T


def lanes(rows, width):
    return lax.broadcasted_iota(jnp.int32, (rows, width), 1)


def right(x):
    return pltpu.roll(x, x.shape[1] - 1, 1)


def left(x):
    return pltpu.roll(x, 1, 1)


def rows_of(shape):
    return lax.broadcasted_iota(jnp.int32, shape, 0)


def above(prev, here):
    return pltpu.roll(jnp.where(rows_of(here.shape) == T - 1, prev, here), 1, 0)


def below(here, after):
    return pltpu.roll(jnp.where(rows_of(here.shape) == 0, after, here), T - 1, 0)


def kernel(
    groups,
    tiles,
    base_in,
    depth_in,
    ssh_in,
    cur_in,
    land_ref,
    thick_in,
    ice_ref,
    vel_in,
    stress_in,
    wind_in,
    ssh_out,
    vel_out,
    stress_out,
    vel,
    st,
    wind,
    flow,
    h,
    kk,
    pp,
    qq,
    g,
    x,
    b,
    gd,
    v0,
    v1,
    v2,
    w0,
    w1,
    w2,
    wet,
    cover,
    pack_s,
    pack_r,
    opack_s,
    opack_r,
    sp,
    back,
    top_in,
    bot_in,
    red_s,
    red_r,
    red2_s,
    red2_r,
    load_sem,
    flow_send,
    flow_recv,
    row_send,
    row_recv,
    col_send,
    col_recv,
    back_send,
    back_recv,
    edge_send,
    edge_recv,
    red_send,
    red_recv,
    red2_send,
    red2_recv,
    out_sem,
):
    gi = lax.axis_index("grp")
    ti = lax.axis_index("tile")
    rows, cols = thick_in.shape[1], thick_in.shape[2]
    orows = base_in.shape[0]
    wide = cols + L
    end = TOP + rows
    oend = TOP + orows

    loads = []

    def load(src, dst):
        copy = pltpu.make_async_copy(src, dst, load_sem.at[len(loads)])
        copy.start()
        loads.append(copy)
        return copy

    load_thick = load(thick_in, h.at[:, TOP:end, 0:cols])
    load_depth = load(depth_in, g.at[TOP:oend, 0:cols])
    load_x = load(ssh_in, x.at[TOP:oend, 0:cols])
    load_b = load(base_in, b.at[TOP:oend, 0:cols])
    load_vel = load(vel_in, vel.at[:, :, TOP:end, 0:cols])
    load_st = load(stress_in, st.at[:, :, TOP:end, 0:cols])
    load_wind = load(wind_in, wind.at[:, :, TOP:end, 0:cols])

    def clear(ref, top, last, total):
        ref[..., 0:top, :] = jnp.zeros(ref.shape[:-2] + (top, wide), F32)
        ref[..., last:total, :] = jnp.zeros(ref.shape[:-2] + (total - last, wide), F32)
        ref[..., top:last, cols:wide] = jnp.zeros(ref.shape[:-2] + (last - top, L), F32)

    for ref in (vel, st, wind, flow, h):
        clear(ref, TOP, end, end + TOP)
    for ref in (g, x, b):
        clear(ref, TOP, oend, oend + TOP)
    for ref in (pack_r, opack_r):
        ref[...] = jnp.zeros_like(ref)

    barrier = pltpu.get_barrier_semaphore()
    for d in range(1, groups):
        pl.semaphore_signal(
            barrier, inc=1, device_id=(lax.rem(gi + d, groups), ti), device_id_type=MESH
        )
    for d in range(1, tiles):
        pl.semaphore_signal(
            barrier, inc=1, device_id=(gi, lax.rem(ti + d, tiles)), device_id_type=MESH
        )

    def blocks(ref, out, count):
        width = ref.shape[-1]
        row = lax.broadcasted_iota(jnp.int32, (width, cols), 0)
        spread = (row == lax.shift_right_logical(lanes(width, cols), 3)).astype(F32)
        values = ref[...].reshape((count, width)).astype(F32)
        out[...] = jnp.dot(values, spread, preferred_element_type=F32)

    blocks(land_ref, wet, land_ref.shape[0])
    for c in range(2):
        row = lax.broadcasted_iota(jnp.int32, (cols // BS, cols), 0)
        spread = (row == lax.shift_right_logical(lanes(cols // BS, cols), 3)).astype(F32)
        cover[c] = jnp.dot(ice_ref[c].astype(F32), spread, preferred_element_type=F32)

    pl.semaphore_wait(barrier, groups + tiles - 2)

    def flow_copy(cap, target):
        lo = max(0, rows * target - T)
        hi = min(rows * groups, rows * target + rows + T)
        start = TOP + lo - rows * target
        src = cur_in.at[:, lo:hi, :]
        dst = flow.at[:, cap, start : start + hi - lo, 0:cols]
        return src, dst

    homes = (0, groups - 1)
    for cap, home in enumerate(homes):

        @pl.when(gi == home)
        def _():
            order = sorted(range(groups), key=lambda k: -abs(k - home))
            for target in order:
                src, dst = flow_copy(cap, target)
                if target == home:
                    pltpu.make_async_copy(src, dst, flow_recv.at[cap]).start()
                else:
                    pltpu.make_async_remote_copy(
                        src_ref=src,
                        dst_ref=dst,
                        send_sem=flow_send.at[target],
                        recv_sem=flow_recv.at[cap],
                        device_id=(target, ti),
                        device_id_type=MESH,
                    ).start()

    def row_copies(which):
        out = []
        fields = (
            (vel_in, vel, rows, end),
            (stress_in, st, rows, end),
            (wind_in, wind, rows, end),
            (ssh_in, x, orows, oend),
            (base_in, b, orows, oend),
            (h, h, None, end),
            (g, g, None, oend),
        )
        for k, (src, dst, length, last) in enumerate(fields):
            if k not in which:
                continue
            origin = TOP if length is None else 0
            span = (last - TOP) if length is None else length
            lead = (slice(None),) * (len(src.shape) - 2)
            for way in range(2):
                from_row = origin + span - T if way == 0 else origin
                to_row = TOP - T if way == 0 else last
                out.append(
                    (
                        way,
                        pltpu.make_async_remote_copy(
                            src_ref=src.at[lead + (slice(from_row, from_row + T), slice(0, cols))],
                            dst_ref=dst.at[lead + (slice(to_row, to_row + T), slice(0, cols))],
                            send_sem=row_send.at[2 * k + way],
                            recv_sem=row_recv.at[2 * k + way],
                            device_id=(
                                lax.rem(gi + (1 if way == 0 else groups - 1), groups),
                                ti,
                            ),
                            device_id_type=MESH,
                        ),
                    )
                )
        return out

    def edge(way, index, count):
        sends = index < count - 1 if way == 0 else index > 0
        receives = index > 0 if way == 0 else index < count - 1
        return sends, receives

    early = row_copies((0, 1, 2))
    for way, copy in early:
        pl.when(edge(way, gi, groups)[0])(copy.start)

    load_thick.wait()

    def cover_chunk(k, _):
        for c in range(2):
            at = (c, pl.ds(pl.multiple_of(TOP + k * T, T), T), pl.ds(0, cols))
            h[at] = h[at] * cover[c, pl.ds(k, 1), :]
        return 0

    lax.fori_loop(0, rows // T, cover_chunk, 0)
    late = row_copies((5,))
    for way, copy in late:
        pl.when(edge(way, gi, groups)[0])(copy.start)
    load_depth.wait()

    def wet_chunk(k, _):
        at = (pl.ds(pl.multiple_of(TOP + k * T, T), T), pl.ds(0, cols))
        g[at] = g[at] * wet[pl.ds(k, 1), :]
        return 0

    lax.fori_loop(0, orows // T, wet_chunk, 0, unroll=4)
    load_vel.wait()
    load_st.wait()
    load_wind.wait()
    load_x.wait()
    load_b.wait()
    for way, copy in early + late:
        pl.when(edge(way, gi, groups)[1])(copy.wait_recv)

    lane = lanes(T, L)

    def col_copies(src, dst, base):
        out = []
        for way in range(2):
            out.append(
                (
                    way,
                    pltpu.make_async_remote_copy(
                        src_ref=src.at[way],
                        dst_ref=dst.at[way],
                        send_sem=col_send.at[base + way],
                        recv_sem=col_recv.at[base + way],
                        device_id=(gi, lax.rem(ti + (1 if way == 0 else tiles - 1), tiles)),
                        device_id_type=MESH,
                    ),
                )
            )
        return out

    def packed(values):
        after = jnp.zeros((T, L), F32)
        before = jnp.zeros((T, L), F32)
        for f, (first, last) in enumerate(values):
            here = (lane >= W * f) & (lane < W * f + W)
            after = jnp.where(here, pltpu.roll(last, (W * f + W) % L, 1), after)
            before = jnp.where(here, pltpu.roll(first, W * f, 1) if f else first, before)
        return after, before

    def unpacked(from_before, from_after, f):
        low = pltpu.roll(from_before, (L - W - W * f) % L, 1)
        high = pltpu.roll(from_after, (L - W * f) % L, 1) if f else from_after
        return jnp.where(lane < W, high, jnp.where(lane >= L - W, low, 0.0))

    ochunks = orows // T + 2
    ichunks = rows // T + 2

    for target in range(groups):

        @pl.when(gi == target)
        def _():
            for cap, home in enumerate(homes):
                src, dst = flow_copy(cap, target)
                if target == home:
                    pltpu.make_async_copy(src, dst, flow_recv.at[cap]).wait()
                else:
                    pltpu.make_async_remote_copy(
                        src_ref=src,
                        dst_ref=dst,
                        send_sem=flow_send.at[target],
                        recv_sem=flow_recv.at[cap],
                        device_id=(home, ti),
                        device_id_type=MESH,
                    ).wait_recv()

    def ice_fields(c):
        return (
            vel.at[0, c],
            vel.at[1, c],
            st.at[0, c],
            st.at[1, c],
            st.at[2, c],
            h.at[c],
            wind.at[0, c],
            wind.at[1, c],
            flow.at[0, c],
            flow.at[1, c],
        )

    def pack_chunk(k, _):
        at = pl.ds(pl.multiple_of(T + k * T, T), T)
        to = pl.ds(pl.multiple_of(k * T, T), T)
        for c in range(2):
            after, before = packed(
                [(ref[at, pl.ds(0, L)], ref[at, pl.ds(cols - L, L)]) for ref in ice_fields(c)]
            )
            pack_s[0, c, to, :] = after
            pack_s[1, c, to, :] = before
        return 0

    lax.fori_loop(0, ichunks, pack_chunk, 0, unroll=2)
    icols = col_copies(pack_s, pack_r, 2)
    for way, copy in icols:
        pl.when(edge(way, ti, tiles)[0])(copy.start)

    for way, copy in icols:
        pl.when(edge(way, ti, tiles)[1])(copy.wait_recv)

    orow = row_copies((3, 4, 6))
    for way, copy in orow:
        pl.when(edge(way, gi, groups)[0])(copy.start)

    def unpack_chunk(k, _):
        at = pl.ds(pl.multiple_of(T + k * T, T), T)
        to = pl.ds(pl.multiple_of(k * T, T), T)
        for c in range(2):
            for f, ref in enumerate(ice_fields(c)):
                ref[at, pl.ds(cols, L)] = unpacked(pack_r[0, c, to, :], pack_r[1, c, to, :], f)
            thick = h[c, at, :]
            mass = thick + 1.0
            inverse = jnp.where(thick > 0.0, 1.0 / (mass + STEP * DRAG), 0.0)
            q = STEP * inverse
            kk[c, at, :] = (RELAX * STRENGTH / (1.0 + RELAX)) * thick
            pp[c, at, :] = mass * inverse
            qq[c, at, :] = q
            for comp in range(2):
                wind[comp, c, at, :] = q * (wind[comp, c, at, :] + DRAG * flow[comp, c, at, :])
        return 0

    lax.fori_loop(0, ichunks, unpack_chunk, 0, unroll=2)

    keep = 1.0 / (1.0 + RELAX)

    def ice_chunk(k, _):
        r = pl.multiple_of(T + k * T, T)
        at = pl.ds(r, T)
        up = pl.ds(pl.multiple_of(r - T, T), T)
        down = pl.ds(pl.multiple_of(r + T, T), T)
        for c in range(2):
            u = vel[0, c, at, :]
            v = vel[1, c, at, :]
            du_dx = below(u, vel[0, c, down, :]) - u
            dv_dx = below(v, vel[1, c, down, :]) - v
            du_dy = right(u) - u
            dv_dy = right(v) - v
            ed = du_dx + dv_dy
            et = du_dx - dv_dy
            es = du_dy + dv_dx
            inverse = lax.rsqrt(ed * ed + et * et + es * es + 1.0)
            k0 = kk[c, at, :]
            k1 = k0 * inverse
            s0 = st[0, c, at, :] * keep + (k1 * ed - k0)
            s1 = st[1, c, at, :] * keep + k1 * et
            s2 = st[2, c, at, :] * keep + k1 * es
            st[0, c, at, :] = s0
            st[1, c, at, :] = s1
            st[2, c, at, :] = s2
            total = s0 + s1
            diff = s0 - s1
            total_up = above(st[0, c, up, :] + st[1, c, up, :], total)
            s2_up = above(st[2, c, up, :], s2)
            fx = 0.5 * (total - total_up) + (s2 - left(s2))
            fy = 0.5 * (diff - left(diff)) + (s2 - s2_up)
            p = pp[c, at, :]
            q = qq[c, at, :]
            vel[0, c, at, :] = p * u + (q * fx + wind[0, c, at, :])
            vel[1, c, at, :] = p * v + (q * fy + wind[1, c, at, :])
        return 0

    def subcycle(n, _):
        return lax.fori_loop(0, ichunks, ice_chunk, 0, unroll=10)

    lax.fori_loop(0, NSUB // 2, subcycle, 0)

    for way, copy in orow:
        pl.when(edge(way, gi, groups)[1])(copy.wait_recv)

    def opack_chunk(k, _):
        at = pl.ds(pl.multiple_of(T + k * T, T), T)
        to = pl.ds(pl.multiple_of(k * T, T), T)
        after, before = packed(
            [(ref[at, pl.ds(0, L)], ref[at, pl.ds(cols - L, L)]) for ref in (g, x, b)]
        )
        opack_s[0, to, :] = after
        opack_s[1, to, :] = before
        return 0

    lax.fori_loop(0, ochunks, opack_chunk, 0, unroll=2)
    ocols = col_copies(opack_s, opack_r, 0)
    for way, copy in ocols:
        pl.when(edge(way, ti, tiles)[0])(copy.start)

    lax.fori_loop(NSUB // 2, NSUB, subcycle, 0)

    sub = lax.broadcasted_iota(jnp.int32, (T, wide), 0)

    def drag(comp, c, where):
        return jnp.where(
            h[c, where, :] > 0.0, DRAG * (vel[comp, c, where, :] - flow[comp, c, where, :]), 0.0
        )

    def drag_chunk(k, _):
        r = pl.multiple_of(TOP + k * T, T)
        to = pl.ds(pl.multiple_of(k * T, T), T)
        for c in range(2):
            d0 = drag(0, c, pl.ds(r, T))
            d0_up = above(drag(0, c, pl.ds(pl.multiple_of(r - T, T), T)), d0)
            d0_up = jnp.where((sub == 0) & (k == 0), 0.0, d0_up)
            d1 = drag(1, c, pl.ds(r, T))
            sp[c, to, :] = (d0 - d0_up) + (d1 - left(d1))
        return 0

    lax.fori_loop(0, rows // T, drag_chunk, 0, unroll=4)
    for c in range(2):
        sp[c, rows : rows + T, :] = drag(0, c, pl.ds(end - T, T))

    outs = [
        pltpu.make_async_copy(vel.at[:, :, TOP:end, 0:cols], vel_out, out_sem.at[0]),
        pltpu.make_async_copy(st.at[:, :, TOP:end, 0:cols], stress_out, out_sem.at[1]),
    ]

    def back_copy(cap, source, target):
        return pltpu.make_async_remote_copy(
            src_ref=sp.at[cap],
            dst_ref=back.at[source],
            send_sem=back_send.at[cap],
            recv_sem=back_recv.at[source],
            device_id=(target, ti),
            device_id_type=MESH,
        )

    def to_top():
        return pltpu.make_async_remote_copy(
            src_ref=sp.at[0, rows - T : rows + T, :],
            dst_ref=top_in,
            send_sem=edge_send.at[0],
            recv_sem=edge_recv.at[0],
            device_id=(1, ti),
            device_id_type=MESH,
        )

    def to_bot():
        return pltpu.make_async_remote_copy(
            src_ref=sp.at[1, 0:T, :],
            dst_ref=bot_in,
            send_sem=edge_send.at[1],
            recv_sem=edge_recv.at[1],
            device_id=(groups - 2, ti),
            device_id_type=MESH,
        )

    pl.when(gi == groups - 1)(lambda: to_top().start())
    pl.when(gi == 0)(lambda: to_bot().start())
    for cap, home in enumerate(homes):
        for source in range(groups):

            @pl.when(gi == source)
            def _():
                if source == home:
                    pltpu.make_async_copy(
                        sp.at[cap], back.at[source], back_recv.at[source]
                    ).start()
                else:
                    back_copy(cap, source, home).start()

    for copy in outs:
        copy.start()

    for way, copy in ocols:
        pl.when(edge(way, ti, tiles)[1])(copy.wait_recv)

    def ounpack_chunk(k, _):
        at = pl.ds(pl.multiple_of(T + k * T, T), T)
        to = pl.ds(pl.multiple_of(k * T, T), T)
        for f, ref in enumerate((g, x, b)):
            ref[at, pl.ds(cols, L)] = unpacked(opack_r[0, to, :], opack_r[1, to, :], f)
        return 0

    lax.fori_loop(0, ochunks, ounpack_chunk, 0, unroll=2)

    zero = jnp.zeros((T, L), F32)

    def fold(value):
        total = value[:, 0:L]
        for j in range(1, cols // L):
            total = total + value[:, j * L : (j + 1) * L]
        return total

    def owned(k):
        return jnp.where((k >= 1) & (k <= orows // T), 1.0, 0.0).astype(F32)

    def around(ref, r):
        middle = ref[pl.ds(r, T), :]
        up = above(ref[pl.ds(pl.multiple_of(r - T, T), T), :], middle)
        down = below(middle, ref[pl.ds(pl.multiple_of(r + T, T), T), :])
        return (up + down) + (left(middle) + right(middle))

    for ref in (w0, w1, w2):
        ref[0:T, :] = jnp.zeros((T, wide), F32)
        ref[oend + T :, :] = jnp.zeros((T, wide), F32)

    def pre_chunk(k, _):
        r = pl.multiple_of(T + k * T, T)
        at = pl.ds(r, T)
        up, down = pl.ds(pl.multiple_of(r - T, T), T), pl.ds(pl.multiple_of(r + T, T), T)
        g0, gu, gw = g[at, :], g[up, :], g[down, :]
        x_0 = x[at, :]
        gx = g0 * x_0
        g_near = (above(gu, g0) + below(g0, gw)) + (left(g0) + right(g0))
        diag = DAMP + g0 * g_near
        near = (above(gu * x[up, :], gx) + below(gx, gw * x[down, :])) + (left(gx) + right(gx))
        b[at, :] = jnp.where(g0 > 0.0, b[at, :], 0.0) - diag * x_0 + g0 * near
        inverse = 1.0 / diag
        v2[at, :] = inverse
        gd[at, :] = g0 * inverse
        return 0

    lax.fori_loop(0, ochunks, pre_chunk, 0, unroll=2)

    def add(at, value):
        b[at, :] = b[at, :] + jnp.where(g[at, :] > 0.0, value, 0.0)

    for cap, home in enumerate(homes):

        @pl.when(gi == home)
        def _():
            for source in range(groups):
                if source == home:
                    pltpu.make_async_copy(
                        sp.at[cap], back.at[source], back_recv.at[source]
                    ).wait()
                else:
                    back_copy(cap, source, source).wait_recv()
            for source in range(groups):

                def add_chunk(k, _):
                    at = pl.ds(pl.multiple_of(TOP + source * rows + k * T, T), T)
                    add(at, back[source, pl.ds(pl.multiple_of(k * T, T), T), :])
                    return 0

                lax.fori_loop(0, rows // T, add_chunk, 0, unroll=4)
            for source in range(groups):
                row = TOP + (source + 1) * rows
                add(slice(row, row + 1), -back[source, rows + T - 1 : rows + T, :])

    @pl.when(gi == 1)
    def _():
        to_top().wait_recv()
        add(slice(T, TOP), top_in[0:T, :])
        add(slice(TOP, TOP + 1), -top_in[2 * T - 1 : 2 * T, :])

    @pl.when(gi == groups - 2)
    def _():
        to_bot().wait_recv()
        add(slice(oend, oend + T), bot_in[...])

    def first_chunk(k, sums):
        at = pl.ds(pl.multiple_of(T + k * T, T), T)
        r0 = b[at, :]
        z = r0 * v2[at, :]
        v0[at, :] = z
        w0[at, :] = g[at, :] * z
        return sums + owned(k) * fold(r0 * z)

    m0 = lax.fori_loop(0, ochunks, first_chunk, zero, unroll=2)

    def power(w_from, v_to, w_to):
        def chunk(k, sums):
            r = pl.multiple_of(T + k * T, T)
            at = pl.ds(r, T)
            near = around(w_from, r)
            v = gd[at, :] * near
            w = g[at, :] * v
            v_to[at, :] = v
            w_to[at, :] = w
            own = owned(k)
            return (
                sums[0] + own * fold(w_from[at, :] * near),
                sums[1] + own * fold(w * near),
            )

        return lax.fori_loop(0, ochunks, chunk, (zero, zero), unroll=2)

    m1, m2 = power(w0, v1, w1)
    m3, m4 = power(w1, v2, w2)

    def last_chunk(k, sums):
        r = pl.multiple_of(TOP + k * T, T)
        return sums + fold(w2[pl.ds(r, T), :] * around(w2, r))

    m5 = lax.fori_loop(0, orows // T, last_chunk, zero, unroll=2)

    row = lax.broadcasted_iota(jnp.int32, (T, L), 0)
    moments = zero
    for k, m in enumerate((m0, m1, m2, m3, m4, m5)):
        moments = jnp.where(row == k, jnp.sum(m, axis=0, keepdims=True), moments)

    def all_reduce(value, src, dst, send, recv, index, count, device):
        src[...] = value
        for d in range(1, count):
            pltpu.make_async_remote_copy(
                src_ref=src,
                dst_ref=dst.at[d],
                send_sem=send.at[d],
                recv_sem=recv.at[d],
                device_id=device(lax.rem(index + d, count)),
                device_id_type=MESH,
            ).start()
        for d in range(1, count):
            copy = pltpu.make_async_remote_copy(
                src_ref=src,
                dst_ref=dst.at[d],
                send_sem=send.at[d],
                recv_sem=recv.at[d],
                device_id=device(lax.rem(index + d, count)),
                device_id_type=MESH,
            )
            copy.wait()
        for d in range(1, count):
            value = value + dst[d]
        return value

    moments = all_reduce(
        moments, red_s, red_r, red_send, red_recv, ti, tiles, lambda k: (gi, k)
    )
    moments = all_reduce(
        moments, red2_s, red2_r, red2_send, red2_recv, gi, groups, lambda k: (k, ti)
    )
    total = jnp.sum(moments, axis=1, keepdims=True)
    nu = [total[k : k + 1, :] for k in range(6)]
    a = [nu[k] - nu[k + 1] for k in range(5)]

    tiny = 1e-12

    def safe(value, scale):
        ok = value > tiny * scale
        return jnp.where(ok, 1.0 / jnp.where(ok, value, 1.0), 0.0)

    i0 = safe(a[0], 0.0 * a[0])
    l10, l20 = a[1] * i0, a[2] * i0
    d1 = a[2] - l10 * a[1]
    i1 = safe(d1, a[2])
    e21 = a[3] - l20 * a[1]
    l21 = e21 * i1
    d2 = a[4] - l20 * a[2] - l21 * e21
    i2 = safe(d2, a[4])
    y0 = nu[0]
    y1 = nu[1] - l10 * y0
    y2 = nu[2] - l20 * y0 - l21 * y1
    c2 = y2 * i2
    c1 = y1 * i1 - l21 * c2
    c0 = y0 * i0 - l10 * c1 - l20 * c2

    def final_chunk(k, _):
        at = (pl.ds(pl.multiple_of(TOP + k * T, T), T), pl.ds(0, cols))
        x[at] = x[at] + (c0 * v0[at] + (c1 * v1[at] + c2 * v2[at]))
        return 0

    lax.fori_loop(0, orows // T, final_chunk, 0, unroll=4)
    last = pltpu.make_async_copy(x.at[TOP:oend, 0:cols], ssh_out, out_sem.at[2])
    last.start()

    for way, copy in early + late + orow:
        pl.when(edge(way, gi, groups)[0])(copy.wait_send)
    for way, copy in ocols + icols:
        pl.when(edge(way, ti, tiles)[0])(copy.wait_send)
    for cap, home in enumerate(homes):

        @pl.when(gi == home)
        def _():
            for target in range(groups):
                if target != home:
                    src, dst = flow_copy(cap, target)
                    pltpu.make_async_remote_copy(
                        src_ref=src,
                        dst_ref=dst,
                        send_sem=flow_send.at[target],
                        recv_sem=flow_recv.at[cap],
                        device_id=(target, ti),
                        device_id_type=MESH,
                    ).wait_send()

        @pl.when(gi != home)
        def _():
            back_copy(cap, 0, home).wait_send()

    pl.when(gi == groups - 1)(lambda: to_top().wait_send())
    pl.when(gi == 0)(lambda: to_bot().wait_send())
    for copy in outs:
        copy.wait()
    last.wait()


def step(groups, tiles, *args):
    base_rhs, thick, ice_vel, ice_stress = args[0], args[5], args[7], args[8]
    orows, cols = base_rhs.shape
    rows = thick.shape[1]
    irows = rows + 2 * TOP
    erows = orows + 2 * TOP
    wide = cols + L
    any_spec = pl.BlockSpec(memory_space=pl.ANY)
    hbm = pl.BlockSpec(memory_space=pltpu.HBM)
    vmem = pl.BlockSpec(memory_space=pltpu.VMEM)
    dma = pltpu.SemaphoreType.DMA
    ice = pltpu.VMEM((2, irows, wide), F32)
    ocean = pltpu.VMEM((erows, wide), F32)
    return pl.pallas_call(
        functools.partial(kernel, groups, tiles),
        out_shape=(
            jax.ShapeDtypeStruct(base_rhs.shape, F32),
            jax.ShapeDtypeStruct(ice_vel.shape, F32),
            jax.ShapeDtypeStruct(ice_stress.shape, F32),
        ),
        in_specs=[hbm] * 4 + [vmem, hbm, vmem] + [hbm] * 3,
        out_specs=(any_spec,) * 3,
        scratch_shapes=[
            pltpu.VMEM((2, 2, irows, wide), F32),
            pltpu.VMEM((3, 2, irows, wide), F32),
            pltpu.VMEM((2, 2, irows, wide), F32),
            pltpu.VMEM((2, 2, irows, wide), F32),
            ice,
            ice,
            ice,
            ice,
        ]
        + [ocean] * 10
        + [
            pltpu.VMEM((orows // BS, cols), F32),
            pltpu.VMEM((2, rows // BS, cols), F32),
            pltpu.VMEM((2, 2, rows + 2 * T, L), F32),
            pltpu.VMEM((2, 2, rows + 2 * T, L), F32),
            pltpu.VMEM((2, orows + 2 * T, L), F32),
            pltpu.VMEM((2, orows + 2 * T, L), F32),
            pltpu.VMEM((2, rows + T, wide), F32),
            pltpu.VMEM((groups, rows + T, wide), F32),
            pltpu.VMEM((2 * T, wide), F32),
            pltpu.VMEM((T, wide), F32),
            pltpu.VMEM((T, L), F32),
            pltpu.VMEM((tiles, T, L), F32),
            pltpu.VMEM((T, L), F32),
            pltpu.VMEM((groups, T, L), F32),
            dma((7,)),
            dma((groups,)),
            dma((2,)),
            dma((14,)),
            dma((14,)),
            dma((4,)),
            dma((4,)),
            dma((2,)),
            dma((groups,)),
            dma((2,)),
            dma((2,)),
            dma((tiles,)),
            dma((tiles,)),
            dma((groups,)),
            dma((groups,)),
            dma((3,)),
        ],
        compiler_params=pltpu.CompilerParams(
            collective_id=0, has_side_effects=True, vmem_limit_bytes=67_043_328
        ),
    )(*args)


def solution(mesh):
    grid = P("grp", "tile")
    plane = P(None, "grp", "tile")
    stack = P(None, None, "grp", "tile")
    return jax.shard_map(
        functools.partial(step, mesh.shape["grp"], mesh.shape["tile"]),
        mesh=mesh,
        in_specs=(grid, grid, grid, plane, grid, plane, plane, stack, stack, stack),
        out_specs=(grid, stack, stack),
        check_vma=False,
    )
```

```python
import functools

import jax
import jax.numpy as jnp
from jax import lax
from jax.experimental import pallas as pl
from jax.experimental.pallas import tpu as pltpu
from jax.sharding import PartitionSpec as P

BS = 8
NSUB = 8

DAMP = 0.05
RELAX = 0.2
STRENGTH = 0.5
DRAG = 1.0
STEP = 0.5

MESH = pl.DeviceIdType.MESH
F32 = jnp.float32
T = 8
L = 128
W = 12
TOP = 2 * T


def lanes(rows, width):
    return lax.broadcasted_iota(jnp.int32, (rows, width), 1)


def right(x):
    return pltpu.roll(x, x.shape[1] - 1, 1)


def left(x):
    return pltpu.roll(x, 1, 1)


def rows_of(shape):
    return lax.broadcasted_iota(jnp.int32, shape, 0)


def above(prev, here):
    return pltpu.roll(jnp.where(rows_of(here.shape) == T - 1, prev, here), 1, 0)


def below(here, after):
    return pltpu.roll(jnp.where(rows_of(here.shape) == 0, after, here), T - 1, 0)


def kernel(
    groups,
    tiles,
    base_in,
    depth_in,
    ssh_in,
    cur_in,
    land_ref,
    thick_in,
    ice_ref,
    vel_in,
    stress_in,
    wind_in,
    ssh_out,
    vel_out,
    stress_out,
    vel,
    st,
    wind,
    flow,
    h,
    kk,
    pp,
    qq,
    g,
    x,
    b,
    gd,
    v0,
    v1,
    v2,
    w0,
    w1,
    w2,
    wet,
    cover,
    pack_s,
    pack_r,
    opack_s,
    opack_r,
    sp,
    back,
    top_in,
    bot_in,
    red_s,
    red_r,
    red2_s,
    red2_r,
    load_sem,
    flow_send,
    flow_recv,
    row_send,
    row_recv,
    col_send,
    col_recv,
    back_send,
    back_recv,
    edge_send,
    edge_recv,
    red_send,
    red_recv,
    red2_send,
    red2_recv,
    out_sem,
):
    gi = lax.axis_index("grp")
    ti = lax.axis_index("tile")
    rows, cols = thick_in.shape[1], thick_in.shape[2]
    orows = base_in.shape[0]
    wide = cols + L
    end = TOP + rows
    oend = TOP + orows

    loads = []

    def load(src, dst):
        copy = pltpu.make_async_copy(src, dst, load_sem.at[len(loads)])
        copy.start()
        loads.append(copy)
        return copy

    load_thick = load(thick_in, h.at[:, TOP:end, 0:cols])
    load_depth = load(depth_in, g.at[TOP:oend, 0:cols])
    load_x = load(ssh_in, x.at[TOP:oend, 0:cols])
    load_b = load(base_in, b.at[TOP:oend, 0:cols])
    load_vel = load(vel_in, vel.at[:, :, TOP:end, 0:cols])
    load_st = load(stress_in, st.at[:, :, TOP:end, 0:cols])
    load_wind = load(wind_in, wind.at[:, :, TOP:end, 0:cols])

    def clear(ref, top, last, total):
        ref[..., 0:top, :] = jnp.zeros(ref.shape[:-2] + (top, wide), F32)
        ref[..., last:total, :] = jnp.zeros(ref.shape[:-2] + (total - last, wide), F32)
        ref[..., top:last, cols:wide] = jnp.zeros(ref.shape[:-2] + (last - top, L), F32)

    for ref in (vel, st, wind, flow, h):
        clear(ref, TOP, end, end + TOP)
    for ref in (g, x, b):
        clear(ref, TOP, oend, oend + TOP)
    for ref in (pack_r, opack_r):
        ref[...] = jnp.zeros_like(ref)

    barrier = pltpu.get_barrier_semaphore()
    for d in range(1, groups):
        pl.semaphore_signal(
            barrier, inc=1, device_id=(lax.rem(gi + d, groups), ti), device_id_type=MESH
        )
    for d in range(1, tiles):
        pl.semaphore_signal(
            barrier, inc=1, device_id=(gi, lax.rem(ti + d, tiles)), device_id_type=MESH
        )

    def blocks(ref, out, count):
        width = ref.shape[-1]
        row = lax.broadcasted_iota(jnp.int32, (width, cols), 0)
        spread = (row == lax.shift_right_logical(lanes(width, cols), 3)).astype(F32)
        values = ref[...].reshape((count, width)).astype(F32)
        out[...] = jnp.dot(values, spread, preferred_element_type=F32)

    blocks(land_ref, wet, land_ref.shape[0])
    for c in range(2):
        row = lax.broadcasted_iota(jnp.int32, (cols // BS, cols), 0)
        spread = (row == lax.shift_right_logical(lanes(cols // BS, cols), 3)).astype(F32)
        cover[c] = jnp.dot(ice_ref[c].astype(F32), spread, preferred_element_type=F32)

    pl.semaphore_wait(barrier, groups + tiles - 2)

    def flow_copy(cap, target):
        lo = max(0, rows * target - T)
        hi = min(rows * groups, rows * target + rows + T)
        start = TOP + lo - rows * target
        src = cur_in.at[:, lo:hi, :]
        dst = flow.at[:, cap, start : start + hi - lo, 0:cols]
        return src, dst

    homes = (0, groups - 1)
    for cap, home in enumerate(homes):

        @pl.when(gi == home)
        def _():
            order = sorted(range(groups), key=lambda k: -abs(k - home))
            for target in order:
                src, dst = flow_copy(cap, target)
                if target == home:
                    pltpu.make_async_copy(src, dst, flow_recv.at[cap]).start()
                else:
                    pltpu.make_async_remote_copy(
                        src_ref=src,
                        dst_ref=dst,
                        send_sem=flow_send.at[target],
                        recv_sem=flow_recv.at[cap],
                        device_id=(target, ti),
                        device_id_type=MESH,
                    ).start()

    def row_copies(which):
        out = []
        fields = (
            (vel_in, vel, rows, end),
            (stress_in, st, rows, end),
            (wind_in, wind, rows, end),
            (ssh_in, x, orows, oend),
            (base_in, b, orows, oend),
            (h, h, None, end),
            (g, g, None, oend),
        )
        for k, (src, dst, length, last) in enumerate(fields):
            if k not in which:
                continue
            origin = TOP if length is None else 0
            span = (last - TOP) if length is None else length
            lead = (slice(None),) * (len(src.shape) - 2)
            for way in range(2):
                from_row = origin + span - T if way == 0 else origin
                to_row = TOP - T if way == 0 else last
                out.append(
                    (
                        way,
                        pltpu.make_async_remote_copy(
                            src_ref=src.at[lead + (slice(from_row, from_row + T), slice(0, cols))],
                            dst_ref=dst.at[lead + (slice(to_row, to_row + T), slice(0, cols))],
                            send_sem=row_send.at[2 * k + way],
                            recv_sem=row_recv.at[2 * k + way],
                            device_id=(
                                lax.rem(gi + (1 if way == 0 else groups - 1), groups),
                                ti,
                            ),
                            device_id_type=MESH,
                        ),
                    )
                )
        return out

    def edge(way, index, count):
        sends = index < count - 1 if way == 0 else index > 0
        receives = index > 0 if way == 0 else index < count - 1
        return sends, receives

    early = row_copies((0, 1, 2))
    for way, copy in early:
        pl.when(edge(way, gi, groups)[0])(copy.start)

    load_thick.wait()

    def cover_chunk(k, _):
        for c in range(2):
            at = (c, pl.ds(pl.multiple_of(TOP + k * T, T), T), pl.ds(0, cols))
            h[at] = h[at] * cover[c, pl.ds(k, 1), :]
        return 0

    lax.fori_loop(0, rows // T, cover_chunk, 0)
    late = row_copies((5,))
    for way, copy in late:
        pl.when(edge(way, gi, groups)[0])(copy.start)
    load_depth.wait()

    def wet_chunk(k, _):
        at = (pl.ds(pl.multiple_of(TOP + k * T, T), T), pl.ds(0, cols))
        g[at] = g[at] * wet[pl.ds(k, 1), :]
        return 0

    lax.fori_loop(0, orows // T, wet_chunk, 0, unroll=4)
    load_vel.wait()
    load_st.wait()
    load_wind.wait()
    load_x.wait()
    load_b.wait()
    for way, copy in early + late:
        pl.when(edge(way, gi, groups)[1])(copy.wait_recv)

    lane = lanes(T, L)

    def col_copies(src, dst, base):
        out = []
        for way in range(2):
            out.append(
                (
                    way,
                    pltpu.make_async_remote_copy(
                        src_ref=src.at[way],
                        dst_ref=dst.at[way],
                        send_sem=col_send.at[base + way],
                        recv_sem=col_recv.at[base + way],
                        device_id=(gi, lax.rem(ti + (1 if way == 0 else tiles - 1), tiles)),
                        device_id_type=MESH,
                    ),
                )
            )
        return out

    def packed(values):
        after = jnp.zeros((T, L), F32)
        before = jnp.zeros((T, L), F32)
        for f, (first, last) in enumerate(values):
            here = (lane >= W * f) & (lane < W * f + W)
            after = jnp.where(here, pltpu.roll(last, (W * f + W) % L, 1), after)
            before = jnp.where(here, pltpu.roll(first, W * f, 1) if f else first, before)
        return after, before

    def unpacked(from_before, from_after, f):
        low = pltpu.roll(from_before, (L - W - W * f) % L, 1)
        high = pltpu.roll(from_after, (L - W * f) % L, 1) if f else from_after
        return jnp.where(lane < W, high, jnp.where(lane >= L - W, low, 0.0))

    ochunks = orows // T + 2
    ichunks = rows // T + 2

    for target in range(groups):

        @pl.when(gi == target)
        def _():
            for cap, home in enumerate(homes):
                src, dst = flow_copy(cap, target)
                if target == home:
                    pltpu.make_async_copy(src, dst, flow_recv.at[cap]).wait()
                else:
                    pltpu.make_async_remote_copy(
                        src_ref=src,
                        dst_ref=dst,
                        send_sem=flow_send.at[target],
                        recv_sem=flow_recv.at[cap],
                        device_id=(home, ti),
                        device_id_type=MESH,
                    ).wait_recv()

    def ice_fields(c):
        return (
            vel.at[0, c],
            vel.at[1, c],
            st.at[0, c],
            st.at[1, c],
            st.at[2, c],
            h.at[c],
            wind.at[0, c],
            wind.at[1, c],
            flow.at[0, c],
            flow.at[1, c],
        )

    def pack_chunk(k, _):
        at = pl.ds(pl.multiple_of(T + k * T, T), T)
        to = pl.ds(pl.multiple_of(k * T, T), T)
        for c in range(2):
            after, before = packed(
                [(ref[at, pl.ds(0, L)], ref[at, pl.ds(cols - L, L)]) for ref in ice_fields(c)]
            )
            pack_s[0, c, to, :] = after
            pack_s[1, c, to, :] = before
        return 0

    lax.fori_loop(0, ichunks, pack_chunk, 0, unroll=5)
    icols = col_copies(pack_s, pack_r, 2)
    for way, copy in icols:
        pl.when(edge(way, ti, tiles)[0])(copy.start)

    for way, copy in icols:
        pl.when(edge(way, ti, tiles)[1])(copy.wait_recv)

    orow = row_copies((3, 4, 6))
    for way, copy in orow:
        pl.when(edge(way, gi, groups)[0])(copy.start)

    def unpack_chunk(k, _):
        at = pl.ds(pl.multiple_of(T + k * T, T), T)
        to = pl.ds(pl.multiple_of(k * T, T), T)
        for c in range(2):
            for f, ref in enumerate(ice_fields(c)):
                ref[at, pl.ds(cols, L)] = unpacked(pack_r[0, c, to, :], pack_r[1, c, to, :], f)
            thick = h[c, at, :]
            mass = thick + 1.0
            inverse = jnp.where(thick > 0.0, 1.0 / (mass + STEP * DRAG), 0.0)
            q = STEP * inverse
            kk[c, at, :] = (RELAX * STRENGTH / (1.0 + RELAX)) * thick
            pp[c, at, :] = mass * inverse
            qq[c, at, :] = q
            for comp in range(2):
                wind[comp, c, at, :] = q * (wind[comp, c, at, :] + DRAG * flow[comp, c, at, :])
        return 0

    lax.fori_loop(0, ichunks, unpack_chunk, 0, unroll=5)

    keep = 1.0 / (1.0 + RELAX)

    def ice_chunk(k, _):
        r = pl.multiple_of(T + k * T, T)
        at = pl.ds(r, T)
        up = pl.ds(pl.multiple_of(r - T, T), T)
        down = pl.ds(pl.multiple_of(r + T, T), T)
        for c in range(2):
            u = vel[0, c, at, :]
            v = vel[1, c, at, :]
            du_dx = below(u, vel[0, c, down, :]) - u
            dv_dx = below(v, vel[1, c, down, :]) - v
            du_dy = right(u) - u
            dv_dy = right(v) - v
            ed = du_dx + dv_dy
            et = du_dx - dv_dy
            es = du_dy + dv_dx
            inverse = lax.rsqrt(ed * ed + et * et + es * es + 1.0)
            k0 = kk[c, at, :]
            k1 = k0 * inverse
            s0 = st[0, c, at, :] * keep + (k1 * ed - k0)
            s1 = st[1, c, at, :] * keep + k1 * et
            s2 = st[2, c, at, :] * keep + k1 * es
            st[0, c, at, :] = s0
            st[1, c, at, :] = s1
            st[2, c, at, :] = s2
            total = s0 + s1
            diff = s0 - s1
            total_up = above(st[0, c, up, :] + st[1, c, up, :], total)
            s2_up = above(st[2, c, up, :], s2)
            fx = 0.5 * (total - total_up) + (s2 - left(s2))
            fy = 0.5 * (diff - left(diff)) + (s2 - s2_up)
            p = pp[c, at, :]
            q = qq[c, at, :]
            vel[0, c, at, :] = p * u + (q * fx + wind[0, c, at, :])
            vel[1, c, at, :] = p * v + (q * fy + wind[1, c, at, :])
        return 0

    def subcycle(n, _):
        return lax.fori_loop(0, ichunks, ice_chunk, 0, unroll=10)

    lax.fori_loop(0, NSUB // 2, subcycle, 0)

    for way, copy in orow:
        pl.when(edge(way, gi, groups)[1])(copy.wait_recv)

    def opack_chunk(k, _):
        at = pl.ds(pl.multiple_of(T + k * T, T), T)
        to = pl.ds(pl.multiple_of(k * T, T), T)
        after, before = packed(
            [(ref[at, pl.ds(0, L)], ref[at, pl.ds(cols - L, L)]) for ref in (g, x, b)]
        )
        opack_s[0, to, :] = after
        opack_s[1, to, :] = before
        return 0

    lax.fori_loop(0, ochunks, opack_chunk, 0, unroll=17)
    ocols = col_copies(opack_s, opack_r, 0)
    for way, copy in ocols:
        pl.when(edge(way, ti, tiles)[0])(copy.start)

    lax.fori_loop(NSUB // 2, NSUB, subcycle, 0)

    sub = lax.broadcasted_iota(jnp.int32, (T, wide), 0)

    def drag(comp, c, where):
        return jnp.where(
            h[c, where, :] > 0.0, DRAG * (vel[comp, c, where, :] - flow[comp, c, where, :]), 0.0
        )

    def drag_chunk(k, _):
        r = pl.multiple_of(TOP + k * T, T)
        to = pl.ds(pl.multiple_of(k * T, T), T)
        for c in range(2):
            d0 = drag(0, c, pl.ds(r, T))
            d0_up = above(drag(0, c, pl.ds(pl.multiple_of(r - T, T), T)), d0)
            d0_up = jnp.where((sub == 0) & (k == 0), 0.0, d0_up)
            d1 = drag(1, c, pl.ds(r, T))
            sp[c, to, :] = (d0 - d0_up) + (d1 - left(d1))
        return 0

    lax.fori_loop(0, rows // T, drag_chunk, 0, unroll=4)
    for c in range(2):
        sp[c, rows : rows + T, :] = drag(0, c, pl.ds(end - T, T))

    outs = [
        pltpu.make_async_copy(vel.at[:, :, TOP:end, 0:cols], vel_out, out_sem.at[0]),
        pltpu.make_async_copy(st.at[:, :, TOP:end, 0:cols], stress_out, out_sem.at[1]),
    ]

    def back_copy(cap, source, target):
        return pltpu.make_async_remote_copy(
            src_ref=sp.at[cap],
            dst_ref=back.at[source],
            send_sem=back_send.at[cap],
            recv_sem=back_recv.at[source],
            device_id=(target, ti),
            device_id_type=MESH,
        )

    def to_top():
        return pltpu.make_async_remote_copy(
            src_ref=sp.at[0, rows - T : rows + T, :],
            dst_ref=top_in,
            send_sem=edge_send.at[0],
            recv_sem=edge_recv.at[0],
            device_id=(1, ti),
            device_id_type=MESH,
        )

    def to_bot():
        return pltpu.make_async_remote_copy(
            src_ref=sp.at[1, 0:T, :],
            dst_ref=bot_in,
            send_sem=edge_send.at[1],
            recv_sem=edge_recv.at[1],
            device_id=(groups - 2, ti),
            device_id_type=MESH,
        )

    pl.when(gi == groups - 1)(lambda: to_top().start())
    pl.when(gi == 0)(lambda: to_bot().start())
    for cap, home in enumerate(homes):
        for source in range(groups):

            @pl.when(gi == source)
            def _():
                if source == home:
                    pltpu.make_async_copy(
                        sp.at[cap], back.at[source], back_recv.at[source]
                    ).start()
                else:
                    back_copy(cap, source, home).start()

    for copy in outs:
        copy.start()

    for way, copy in ocols:
        pl.when(edge(way, ti, tiles)[1])(copy.wait_recv)

    def ounpack_chunk(k, _):
        at = pl.ds(pl.multiple_of(T + k * T, T), T)
        to = pl.ds(pl.multiple_of(k * T, T), T)
        for f, ref in enumerate((g, x, b)):
            ref[at, pl.ds(cols, L)] = unpacked(opack_r[0, to, :], opack_r[1, to, :], f)
        return 0

    lax.fori_loop(0, ochunks, ounpack_chunk, 0, unroll=17)

    zero = jnp.zeros((T, L), F32)

    def fold(value):
        total = value[:, 0:L]
        for j in range(1, cols // L):
            total = total + value[:, j * L : (j + 1) * L]
        return total

    def owned(k):
        return jnp.where((k >= 1) & (k <= orows // T), 1.0, 0.0).astype(F32)

    def around(ref, r):
        middle = ref[pl.ds(r, T), :]
        up = above(ref[pl.ds(pl.multiple_of(r - T, T), T), :], middle)
        down = below(middle, ref[pl.ds(pl.multiple_of(r + T, T), T), :])
        return (up + down) + (left(middle) + right(middle))

    for ref in (w0, w1, w2):
        ref[0:T, :] = jnp.zeros((T, wide), F32)
        ref[oend + T :, :] = jnp.zeros((T, wide), F32)

    def pre_chunk(k, _):
        r = pl.multiple_of(T + k * T, T)
        at = pl.ds(r, T)
        up, down = pl.ds(pl.multiple_of(r - T, T), T), pl.ds(pl.multiple_of(r + T, T), T)
        g0, gu, gw = g[at, :], g[up, :], g[down, :]
        x_0 = x[at, :]
        gx = g0 * x_0
        g_near = (above(gu, g0) + below(g0, gw)) + (left(g0) + right(g0))
        diag = DAMP + g0 * g_near
        near = (above(gu * x[up, :], gx) + below(gx, gw * x[down, :])) + (left(gx) + right(gx))
        b[at, :] = jnp.where(g0 > 0.0, b[at, :], 0.0) - diag * x_0 + g0 * near
        inverse = 1.0 / diag
        v2[at, :] = inverse
        gd[at, :] = g0 * inverse
        return 0

    lax.fori_loop(0, ochunks, pre_chunk, 0, unroll=2)

    def add(at, value):
        b[at, :] = b[at, :] + jnp.where(g[at, :] > 0.0, value, 0.0)

    for cap, home in enumerate(homes):

        @pl.when(gi == home)
        def _():
            for source in range(groups):
                if source == home:
                    pltpu.make_async_copy(
                        sp.at[cap], back.at[source], back_recv.at[source]
                    ).wait()
                else:
                    back_copy(cap, source, source).wait_recv()
            for source in range(groups):

                def add_chunk(k, _):
                    at = pl.ds(pl.multiple_of(TOP + source * rows + k * T, T), T)
                    add(at, back[source, pl.ds(pl.multiple_of(k * T, T), T), :])
                    return 0

                lax.fori_loop(0, rows // T, add_chunk, 0, unroll=4)
            for source in range(groups):
                row = TOP + (source + 1) * rows
                add(slice(row, row + 1), -back[source, rows + T - 1 : rows + T, :])

    @pl.when(gi == 1)
    def _():
        to_top().wait_recv()
        add(slice(T, TOP), top_in[0:T, :])
        add(slice(TOP, TOP + 1), -top_in[2 * T - 1 : 2 * T, :])

    @pl.when(gi == groups - 2)
    def _():
        to_bot().wait_recv()
        add(slice(oend, oend + T), bot_in[...])

    def first_chunk(k, sums):
        at = pl.ds(pl.multiple_of(T + k * T, T), T)
        r0 = b[at, :]
        z = r0 * v2[at, :]
        v0[at, :] = z
        w0[at, :] = g[at, :] * z
        return sums + owned(k) * fold(r0 * z)

    m0 = lax.fori_loop(0, ochunks, first_chunk, zero, unroll=2)

    def power(w_from, v_to, w_to):
        def chunk(k, sums):
            r = pl.multiple_of(T + k * T, T)
            at = pl.ds(r, T)
            near = around(w_from, r)
            v = gd[at, :] * near
            w = g[at, :] * v
            v_to[at, :] = v
            w_to[at, :] = w
            own = owned(k)
            return (
                sums[0] + own * fold(w_from[at, :] * near),
                sums[1] + own * fold(w * near),
            )

        return lax.fori_loop(0, ochunks, chunk, (zero, zero), unroll=2)

    m1, m2 = power(w0, v1, w1)
    m3, m4 = power(w1, v2, w2)

    def last_chunk(k, sums):
        r = pl.multiple_of(TOP + k * T, T)
        return sums + fold(w2[pl.ds(r, T), :] * around(w2, r))

    m5 = lax.fori_loop(0, orows // T, last_chunk, zero, unroll=2)

    row = lax.broadcasted_iota(jnp.int32, (T, L), 0)
    moments = zero
    for k, m in enumerate((m0, m1, m2, m3, m4, m5)):
        moments = jnp.where(row == k, jnp.sum(m, axis=0, keepdims=True), moments)

    def all_reduce(value, src, dst, send, recv, index, count, device):
        src[...] = value
        for d in range(1, count):
            pltpu.make_async_remote_copy(
                src_ref=src,
                dst_ref=dst.at[d],
                send_sem=send.at[d],
                recv_sem=recv.at[d],
                device_id=device(lax.rem(index + d, count)),
                device_id_type=MESH,
            ).start()
        for d in range(1, count):
            copy = pltpu.make_async_remote_copy(
                src_ref=src,
                dst_ref=dst.at[d],
                send_sem=send.at[d],
                recv_sem=recv.at[d],
                device_id=device(lax.rem(index + d, count)),
                device_id_type=MESH,
            )
            copy.wait()
        for d in range(1, count):
            value = value + dst[d]
        return value

    moments = all_reduce(
        moments, red_s, red_r, red_send, red_recv, ti, tiles, lambda k: (gi, k)
    )
    moments = all_reduce(
        moments, red2_s, red2_r, red2_send, red2_recv, gi, groups, lambda k: (k, ti)
    )
    total = jnp.sum(moments, axis=1, keepdims=True)
    nu = [total[k : k + 1, :] for k in range(6)]
    a = [nu[k] - nu[k + 1] for k in range(5)]

    tiny = 1e-12

    def safe(value, scale):
        ok = value > tiny * scale
        return jnp.where(ok, 1.0 / jnp.where(ok, value, 1.0), 0.0)

    i0 = safe(a[0], 0.0 * a[0])
    l10, l20 = a[1] * i0, a[2] * i0
    d1 = a[2] - l10 * a[1]
    i1 = safe(d1, a[2])
    e21 = a[3] - l20 * a[1]
    l21 = e21 * i1
    d2 = a[4] - l20 * a[2] - l21 * e21
    i2 = safe(d2, a[4])
    y0 = nu[0]
    y1 = nu[1] - l10 * y0
    y2 = nu[2] - l20 * y0 - l21 * y1
    c2 = y2 * i2
    c1 = y1 * i1 - l21 * c2
    c0 = y0 * i0 - l10 * c1 - l20 * c2

    def final_chunk(k, _):
        at = (pl.ds(pl.multiple_of(TOP + k * T, T), T), pl.ds(0, cols))
        x[at] = x[at] + (c0 * v0[at] + (c1 * v1[at] + c2 * v2[at]))
        return 0

    lax.fori_loop(0, orows // T, final_chunk, 0, unroll=4)
    last = pltpu.make_async_copy(x.at[TOP:oend, 0:cols], ssh_out, out_sem.at[2])
    last.start()

    for way, copy in early + late + orow:
        pl.when(edge(way, gi, groups)[0])(copy.wait_send)
    for way, copy in ocols + icols:
        pl.when(edge(way, ti, tiles)[0])(copy.wait_send)
    for cap, home in enumerate(homes):

        @pl.when(gi == home)
        def _():
            for target in range(groups):
                if target != home:
                    src, dst = flow_copy(cap, target)
                    pltpu.make_async_remote_copy(
                        src_ref=src,
                        dst_ref=dst,
                        send_sem=flow_send.at[target],
                        recv_sem=flow_recv.at[cap],
                        device_id=(target, ti),
                        device_id_type=MESH,
                    ).wait_send()

        @pl.when(gi != home)
        def _():
            back_copy(cap, 0, home).wait_send()

    pl.when(gi == groups - 1)(lambda: to_top().wait_send())
    pl.when(gi == 0)(lambda: to_bot().wait_send())
    for copy in outs:
        copy.wait()
    last.wait()


def deliver(*refs):
    half = len(refs) // 2
    for src, dst in zip(refs[:half], refs[half:]):
        dst[...] = src[...]


def step(groups, tiles, *args):
    base_rhs, thick, ice_vel, ice_stress = args[0], args[5], args[7], args[8]
    orows, cols = base_rhs.shape
    rows = thick.shape[1]
    irows = rows + 2 * TOP
    erows = orows + 2 * TOP
    wide = cols + L
    any_spec = pl.BlockSpec(memory_space=pl.ANY)
    hbm = pl.BlockSpec(memory_space=pltpu.HBM)
    vmem = pl.BlockSpec(memory_space=pltpu.VMEM)
    dma = pltpu.SemaphoreType.DMA
    ice = pltpu.VMEM((2, irows, wide), F32)
    ocean = pltpu.VMEM((erows, wide), F32)
    results = pl.pallas_call(
        functools.partial(kernel, groups, tiles),
        out_shape=(
            jax.ShapeDtypeStruct(base_rhs.shape, F32),
            jax.ShapeDtypeStruct(ice_vel.shape, F32),
            jax.ShapeDtypeStruct(ice_stress.shape, F32),
        ),
        in_specs=[hbm] * 4 + [vmem, hbm, vmem] + [hbm] * 3,
        out_specs=(any_spec,) * 3,
        scratch_shapes=[
            pltpu.VMEM((2, 2, irows, wide), F32),
            pltpu.VMEM((3, 2, irows, wide), F32),
            pltpu.VMEM((2, 2, irows, wide), F32),
            pltpu.VMEM((2, 2, irows, wide), F32),
            ice,
            ice,
            ice,
            ice,
        ]
        + [ocean] * 10
        + [
            pltpu.VMEM((orows // BS, cols), F32),
            pltpu.VMEM((2, rows // BS, cols), F32),
            pltpu.VMEM((2, 2, rows + 2 * T, L), F32),
            pltpu.VMEM((2, 2, rows + 2 * T, L), F32),
            pltpu.VMEM((2, orows + 2 * T, L), F32),
            pltpu.VMEM((2, orows + 2 * T, L), F32),
            pltpu.VMEM((2, rows + T, wide), F32),
            pltpu.VMEM((groups, rows + T, wide), F32),
            pltpu.VMEM((2 * T, wide), F32),
            pltpu.VMEM((T, wide), F32),
            pltpu.VMEM((T, L), F32),
            pltpu.VMEM((tiles, T, L), F32),
            pltpu.VMEM((T, L), F32),
            pltpu.VMEM((groups, T, L), F32),
            dma((7,)),
            dma((groups,)),
            dma((2,)),
            dma((14,)),
            dma((14,)),
            dma((4,)),
            dma((4,)),
            dma((2,)),
            dma((groups,)),
            dma((2,)),
            dma((2,)),
            dma((tiles,)),
            dma((tiles,)),
            dma((groups,)),
            dma((groups,)),
            dma((3,)),
        ],
        compiler_params=pltpu.CompilerParams(
            collective_id=0, has_side_effects=True, vmem_limit_bytes=67_043_328
        ),
    )(*args)
    return pl.pallas_call(
        deliver,
        out_shape=tuple(jax.ShapeDtypeStruct(r.shape, F32) for r in results),
        in_specs=[vmem] * 3,
        out_specs=(vmem,) * 3,
    )(*results)


def solution(mesh):
    grid = P("grp", "tile")
    plane = P(None, "grp", "tile")
    stack = P(None, None, "grp", "tile")
    return jax.shard_map(
        functools.partial(step, mesh.shape["grp"], mesh.shape["tile"]),
        mesh=mesh,
        in_specs=(grid, grid, grid, plane, grid, plane, plane, stack, stack, stack),
        out_specs=(grid, stack, stack),
        check_vma=False,
    )
```
